32 devices in a mesh: dp: 1 (over z), tp: 32 (over x, y, core).
Axes of the slice: x: 4, y: 4, z: 1, core: 2. Of those that a mesh axis runs over, the one named last changes fastest.
The devices are a block of a 4x4x8 slice.
Arguments:
- x: bfloat16 [2048, 4096], P('dp')
- dy: bfloat16 [2048, 4096], P('dp')
- gate: bfloat16 [2048, 16384], P('dp', 'tp')
- up: bfloat16 [2048, 16384], P('dp', 'tp')
- w_gate: bfloat16 [4096, 16384], P(None, 'tp')
- w_up: bfloat16 [4096, 16384], P(None, 'tp')
- w_down: bfloat16 [16384, 4096], P('tp')
Outputs:
- output 1: bfloat16 [2048, 4096], P('dp')
- output 2: bfloat16 [4096, 16384], P('dp', 'tp')
- output 3: bfloat16 [4096, 16384], P('dp', 'tp')
- output 4: bfloat16 [16384, 4096], P(('dp', 'tp'))
All inputs are finite; a program needn't handle non-finite values.
Results may differ from the reference program's by a relative error of at most 0.012.
Values are sent between devices in bfloat16 or wider.
A program may use at most 768 MiB of HBM per device.

```python
import jax
import jax.numpy as jnp

ROWS = 2048
D = 4096
FF = 16384


def act(gate, up):
    return jax.nn.silu(gate) * up


def setup_inputs(seed: int = 0, part: int = 0) -> dict:
    kx, ky, ka, kb, kg, ku, kd = jax.random.split(jax.random.key(seed), 7)
    kx, ky, ka, kb = (jax.random.fold_in(k, part) for k in (kx, ky, ka, kb))
    drawn = {
        "x": jax.random.normal(kx, (ROWS, D), jnp.float32),
        "dy": jax.random.normal(ky, (ROWS, D), jnp.float32),
        "gate": jax.random.normal(ka, (ROWS, FF), jnp.float32),
        "up": jax.random.normal(kb, (ROWS, FF), jnp.float32),
        "w_gate": jax.random.normal(kg, (D, FF), jnp.float32) * D**-0.5,
        "w_up": jax.random.normal(ku, (D, FF), jnp.float32) * D**-0.5,
        "w_down": jax.random.normal(kd, (FF, D), jnp.float32) * FF**-0.5,
    }
    return {k: v.astype(jnp.bfloat16) for k, v in drawn.items()}


def reference(x, dy, gate, up, w_gate, w_up, w_down):
    hidden, back = jax.vjp(act, gate.astype(jnp.float32), up.astype(jnp.float32))
    d_hidden = jnp.dot(dy, w_down.T, preferred_element_type=jnp.float32)
    d_gate, d_up = (g.astype(jnp.bfloat16) for g in back(d_hidden))
    dx = jnp.dot(d_gate, w_gate.T, preferred_element_type=jnp.float32) + jnp.dot(d_up, w_up.T, preferred_element_type=jnp.float32)
    dw_gate = jnp.dot(x.T, d_gate, preferred_element_type=jnp.float32)
    dw_up = jnp.dot(x.T, d_up, preferred_element_type=jnp.float32)
    dw_down = jnp.dot(hidden.astype(jnp.bfloat16).T, dy, preferred_element_type=jnp.float32)
    return tuple(g.astype(jnp.bfloat16) for g in (dx, dw_gate, dw_up, dw_down))
```

```python
import functools
import math

import jax
import jax.numpy as jnp
from jax import lax
from jax.experimental import pallas as pl
from jax.experimental.pallas import tpu as pltpu
from jax.sharding import PartitionSpec as P

MESH = pl.DeviceIdType.MESH
F32 = jnp.float32
BF16 = jnp.bfloat16

ROWS = 256
SPLIT = 2
TILE = 256
LAG = (1, 2, 3, 4, 5, 6, 12, 14, 15, 16)
SLOTS = 4


def nt(a, b):
    return lax.dot_general(a, b, (((1,), (1,)), ((), ())), preferred_element_type=F32)


def tn(a, b):
    return lax.dot_general(a, b, (((0,), (0,)), ((), ())), preferred_element_type=F32)


def kernel(side, x, dy, gate, up, w_gate, w_up, w_down, dx, og, ou, od,
           dyb, gb, ub, dgu, hid, xb, yb, own, own2, far, mid, far2, mid2, relay2,
           w_sem, c_sem, b_sem, send, recv):
    tokens, width = dx.shape
    hidden = od.shape[0]
    half = width // 2
    cu = half // SPLIT
    cw = cu // side
    sub = ROWS // side
    chunks = tokens // ROWS
    units = chunks * SPLIT
    steps = width // TILE

    me = lax.axis_index("tp")
    core = lax.rem(me, 2)
    y = lax.rem(me // 2, side)
    xx = me // (2 * side)
    p1 = xx + core * (y - xx)
    p2 = y + core * (xx - y)

    def device(a, b):
        a, b = lax.rem(a + side, side), lax.rem(b + side, side)
        return ((a + core * (b - a)) * side + b + core * (a - b)) * 2 + core

    right, left = device(p1 + 1, p2), device(p1 - 1, p2)
    right2, left2 = device(p1, p2 + 1), device(p1, p2 - 1)
    partner = me + 1 - 2 * core

    barrier = pltpu.get_barrier_semaphore()
    peers = (partner, right, left, right2, left2)
    for peer in peers:
        pl.semaphore_signal(barrier, inc=1, device_id={"tp": peer}, device_id_type=MESH)

    def load_chunk(r):
        s = lax.rem(r, 2)
        rows = pl.ds(pl.multiple_of(r * ROWS, ROWS), ROWS)
        return (
            pltpu.make_async_copy(dy.at[rows], dyb.at[s], c_sem.at[s, 0]),
            pltpu.make_async_copy(gate.at[rows], gb.at[s], c_sem.at[s, 1]),
            pltpu.make_async_copy(up.at[rows], ub.at[s], c_sem.at[s, 2]),
        )

    def load_tile(j):
        s = lax.rem(j, 2)
        cols = pl.ds(pl.multiple_of(j * TILE, TILE), TILE)
        return (
            pltpu.make_async_copy(x.at[:, cols], xb.at[s], b_sem.at[s, 0]),
            pltpu.make_async_copy(dy.at[:, cols], yb.at[s], b_sem.at[s, 1]),
        )

    load_w = (
        pltpu.make_async_copy(w_down, od, w_sem.at[0]),
        pltpu.make_async_copy(w_gate, og, w_sem.at[1]),
        pltpu.make_async_copy(w_up, ou, w_sem.at[2]),
    )
    for c in load_chunk(0):
        c.start()
    for c in load_w:
        c.start()

    pl.semaphore_wait(barrier, len(peers))

    def rows_of(u, first=0, count=ROWS):
        return pl.ds(pl.multiple_of((u // SPLIT) * ROWS + first, math.gcd(count, 64)), count)

    def base(u, h):
        return h * half + lax.rem(u, SPLIT) * cu

    def piece(u, d):
        q = lax.rem(p1 + d, side)
        return q, pl.ds(pl.multiple_of(base(u, core) + q * cw, cw), cw)

    def ship(src, dst, stage, u, to, kind):
        pltpu.make_async_remote_copy(
            src_ref=src, dst_ref=dst, send_sem=send.at[stage, lax.rem(u, 2) if stage < 5 else 0],
            recv_sem=recv.at[kind, u],
            device_id={"tp": to}, device_id_type=MESH,
        ).start()

    def arrived(ref, kind, u):
        pltpu.make_async_copy(ref, ref, recv.at[kind, u]).wait()

    def amount(rows, cols):
        return dx.at[pl.ds(0, rows), pl.ds(0, cols)]

    def left_with(ref, stage, u):
        pltpu.make_async_copy(ref, ref, send.at[stage, lax.rem(u, 2)]).wait()

    def s0(u):
        r = u // SPLIT
        s = lax.rem(r, 2)
        rows = rows_of(u)

        @pl.when(lax.rem(u, SPLIT) == 0)
        def _():
            @pl.when(r + 1 < chunks)
            def _():
                for c in load_chunk(r + 1):
                    c.start()

            for c in load_chunk(r):
                c.wait()

            @pl.when(r == 0)
            def _():
                load_w[0].wait()

            dh = nt(dyb[s], od[...])
            g = gb[s].astype(F32)
            v = ub[s].astype(F32)
            sig = jax.nn.sigmoid(g)
            silu = g * sig
            hid[:, pl.ds(pl.multiple_of(r * ROWS, ROWS), ROWS)] = (silu * v).T.astype(BF16)
            dgu[rows, hidden:] = (dh * silu).astype(BF16)
            dgu[rows, :hidden] = (dh * v * (sig + silu * (1.0 - sig))).astype(BF16)

            @pl.when(r == 0)
            def _():
                load_w[1].wait()
                load_w[2].wait()

        def term(h):
            cols = pl.ds(pl.multiple_of(base(u, h), cu), cu)
            return nt(dgu[rows, :hidden], og[cols, :]) + nt(dgu[rows, hidden:], ou[cols, :])

        there = dx.at[rows, pl.ds(pl.multiple_of(base(u, 1 - core), cu), cu)]
        there[...] = term(1 - core).astype(BF16)
        ship(there, there, 0, u, partner, 0)
        own[lax.rem(u, SLOTS)] = term(core)

    hr = ROWS // 2

    def s1(u):
        here = dx.at[rows_of(u), pl.ds(pl.multiple_of(base(u, core), cu), cu)]
        arrived(here, 0, u)
        left_with(amount(ROWS, cu), 0, u)
        mine = own.at[lax.rem(u, SLOTS)]
        upper, lower = rows_of(u, 0, hr), rows_of(u, hr, hr)

        def total(d):
            q, cols = piece(u, d)
            at = pl.ds(pl.multiple_of(q * cw, cw), cw)
            return at, cols, mine[:, at] + dx[rows_of(u), cols].astype(F32)

        at, cols, v = total(side // 2)
        dx[rows_of(u), cols] = v.astype(BF16)
        ship(dx.at[upper, cols], far.at[u, 0], 1, u, left, 1)
        ship(dx.at[lower, cols], far.at[u, 1], 1, u, right, 1)
        at, cols, v = total(1)
        dx[upper, cols] = v[:hr].astype(BF16)
        ship(dx.at[upper, cols], mid.at[u, 0], 1, u, right, 2)
        mine[hr:, at] = v[hr:]
        at, cols, v = total(side - 1)
        dx[lower, cols] = v[hr:].astype(BF16)
        ship(dx.at[lower, cols], mid.at[u, 1], 1, u, left, 2)
        mine[:hr, at] = v[:hr]
        at, cols, v = total(0)
        mine[:, at] = v

    def s2(u):
        arrived(far.at[u], 1, u)
        left_with(amount(2 * ROWS, cw), 1, u)
        mine = own.at[lax.rem(u, SLOTS)]
        upper, lower = rows_of(u, 0, hr), rows_of(u, hr, hr)
        q, cols = piece(u, side - 1)
        at = pl.ds(pl.multiple_of(q * cw, cw), cw)
        dx[upper, cols] = (mine[:hr, at] + far[u, 0].astype(F32)).astype(BF16)
        ship(dx.at[upper, cols], mid.at[u, 2], 2, u, left, 2)
        q, cols = piece(u, 1)
        at = pl.ds(pl.multiple_of(q * cw, cw), cw)
        dx[lower, cols] = (mine[hr:, at] + far[u, 1].astype(F32)).astype(BF16)
        ship(dx.at[lower, cols], mid.at[u, 3], 2, u, right, 2)

    hs = sub // 2

    def part(d):
        return pl.multiple_of(lax.rem(p2 + d, side) * sub, sub)

    def s3(u):
        arrived(mid.at[u], 2, u)
        left_with(amount(ROWS, cw), 2, u)
        q, cols = piece(u, 0)
        at = pl.ds(pl.multiple_of(q * cw, cw), cw)
        mine = own.at[lax.rem(u, SLOTS)]
        keep = own2.at[lax.rem(u, SLOTS)]
        keep[:hr] = mine[:hr, at] + mid[u, 0].astype(F32) + mid[u, 2].astype(F32)
        keep[hr:] = mine[hr:, at] + mid[u, 1].astype(F32) + mid[u, 3].astype(F32)

        f = part(side // 2)
        dx[rows_of(u, f, sub), cols] = keep[pl.ds(f, sub)].astype(BF16)
        ship(dx.at[rows_of(u, f, hs), cols], far2.at[u, 0], 3, u, left2, 3)
        ship(dx.at[rows_of(u, f + hs, hs), cols], far2.at[u, 1], 3, u, right2, 3)
        f = part(1)
        dx[rows_of(u, f, hs), cols] = keep[pl.ds(f, hs)].astype(BF16)
        ship(dx.at[rows_of(u, f, hs), cols], mid2.at[u, 0], 3, u, right2, 4)
        f = pl.multiple_of(part(side - 1) + hs, hs)
        dx[rows_of(u, f, hs), cols] = keep[pl.ds(f, hs)].astype(BF16)
        ship(dx.at[rows_of(u, f, hs), cols], mid2.at[u, 1], 3, u, left2, 4)

    def s4(u):
        arrived(far2.at[u], 3, u)
        left_with(amount(2 * sub, cw), 3, u)
        keep = own2.at[lax.rem(u, SLOTS)]
        f = part(side - 1)
        relay2[u, 0] = (keep[pl.ds(f, hs)] + far2[u, 0].astype(F32)).astype(BF16)
        ship(relay2.at[u, 0], mid2.at[u, 2], 4, u, left2, 4)
        f = pl.multiple_of(part(1) + hs, hs)
        relay2[u, 1] = (keep[pl.ds(f, hs)] + far2[u, 1].astype(F32)).astype(BF16)
        ship(relay2.at[u, 1], mid2.at[u, 3], 4, u, right2, 4)

    def s5(u):
        arrived(mid2.at[u], 4, u)
        left_with(amount(sub, cw), 4, u)
        _, cols = piece(u, 0)
        keep = own2.at[lax.rem(u, SLOTS)]
        f = part(0)
        a = keep[pl.ds(f, hs)] + mid2[u, 0].astype(F32) + mid2[u, 2].astype(F32)
        g = pl.multiple_of(f + hs, hs)
        b = keep[pl.ds(g, hs)] + mid2[u, 1].astype(F32) + mid2[u, 3].astype(F32)
        dx[rows_of(u, f, hs), cols] = a.astype(BF16)
        dx[rows_of(u, g, hs), cols] = b.astype(BF16)
        done = dx.at[rows_of(u, f, sub), cols]
        ship(done, done, 5, u, left2, 5)
        ship(done, done, 5, u, right2, 5)

    def s6(u):
        arrived(amount(2 * sub, cw), 5, u)
        _, cols = piece(u, 0)
        a = dx.at[rows_of(u, part(side - 1), hs), cols]
        b = dx.at[rows_of(u, part(1) + hs, hs), cols]
        ship(a, a, 6, u, right2, 6)
        ship(b, b, 6, u, left2, 6)

    def s7(u):
        arrived(amount(sub, cw), 6, u)
        _, cols = piece(u, 0)
        done = dx.at[rows_of(u), cols]
        ship(done, done, 7, u, left, 7)
        ship(done, done, 7, u, right, 7)
        ship(done, done, 7, u, partner, 9)

    def s8(u):
        arrived(amount(2 * ROWS, cw), 7, u)
        _, lcols = piece(u, side - 1)
        _, rcols = piece(u, 1)
        a = dx.at[rows_of(u, 0, hr), lcols]
        b = dx.at[rows_of(u, hr, hr), rcols]
        ship(a, a, 8, u, right, 8)
        ship(b, b, 8, u, left, 8)
        for cols in (lcols, rcols):
            done = dx.at[rows_of(u), cols]
            ship(done, done, 8, u, partner, 9)

    def s9(u):
        arrived(amount(ROWS, cw), 8, u)
        _, cols = piece(u, side // 2)
        done = dx.at[rows_of(u), cols]
        ship(done, done, 9, u, partner, 9)

    def s10(u):
        arrived(amount(ROWS, cu), 9, u)

    def grads(j):
        s = lax.rem(j, 2)

        @pl.when(j + 1 < steps)
        def _():
            for c in load_tile(j + 1):
                c.start()

        for c in load_tile(j):
            c.wait()
        at = pl.ds(pl.multiple_of(j * TILE, TILE), TILE)
        both = tn(xb[s], dgu[...])
        og[at, :] = both[:, :hidden].astype(BF16)
        ou[at, :] = both[:, hidden:].astype(BF16)
        od[:, at] = jnp.dot(hid[...], yb[s], preferred_element_type=F32).astype(BF16)

    total = units + max(LAG[-1], steps)

    def iteration(i, carry):
        pl.when(i < units)(lambda: s0(i))
        for lag, stage in zip(LAG, (s1, s2, s3, s4, s5, s6, s7, s8, s9, s10)):
            pl.when((i >= lag) & (i < units + lag))(functools.partial(stage, i - lag))

        @pl.when(i == units // 2)
        def _():
            for c in load_tile(0):
                c.start()

        pl.when((i >= units) & (i < units + steps))(lambda: grads(i - units))
        return carry

    lax.fori_loop(0, total, iteration, 0)

    for stage, share in ((5, 2), (6, 1), (7, 12), (8, 12), (9, 4)):
        ref = dx.at[:, pl.ds(0, share * width // 32)]
        pltpu.make_async_copy(ref, ref, send.at[stage, 0]).wait()


def solution(mesh):
    side = math.isqrt(mesh.shape["tp"] // 2)

    def step(x, dy, gate, up, w_gate, w_up, w_down):
        tokens, width = x.shape
        hidden = gate.shape[1]
        units = tokens // ROWS * SPLIT
        cu = width // 2 // SPLIT
        cw = cu // side
        sub = ROWS // side
        out = [pltpu.VMEM(a.shape, a.dtype) for a in (x, w_gate, w_up, w_down)]
        dma = pltpu.SemaphoreType.DMA
        return tuple(pl.pallas_call(
            functools.partial(kernel, side),
            out_shape=out,
            in_specs=[pl.BlockSpec(memory_space=pl.ANY)] * 7,
            out_specs=[pl.BlockSpec(memory_space=pltpu.VMEM)] * 4,
            scratch_shapes=[
                pltpu.VMEM((2, ROWS, width), BF16),
                pltpu.VMEM((2, ROWS, hidden), BF16),
                pltpu.VMEM((2, ROWS, hidden), BF16),
                pltpu.VMEM((tokens, 2 * hidden), BF16),
                pltpu.VMEM((hidden, tokens), BF16),
                pltpu.VMEM((2, tokens, TILE), BF16),
                pltpu.VMEM((2, tokens, TILE), BF16),
                pltpu.VMEM((SLOTS, ROWS, cu), F32),
                pltpu.VMEM((SLOTS, ROWS, cw), F32),
                pltpu.VMEM((units, 2, ROWS // 2, cw), BF16),
                pltpu.VMEM((units, 4, ROWS // 2, cw), BF16),
                pltpu.VMEM((units, 2, sub // 2, cw), BF16),
                pltpu.VMEM((units, 4, sub // 2, cw), BF16),
                pltpu.VMEM((units, 2, sub // 2, cw), BF16),
                dma((3,)),
                dma((2, 3)),
                dma((2, 2)),
                dma((10, 2)),
                dma((10, units)),
            ],
            compiler_params=pltpu.CompilerParams(
                collective_id=0, has_side_effects=True, vmem_limit_bytes=34 * 2**20,
            ),
        )(x, dy, gate, up, w_gate, w_up, w_down))

    tokens, columns, rows = P("dp", None), P(None, "tp"), P("tp", None)
    return jax.shard_map(
        step,
        mesh=mesh,
        in_specs=(tokens, tokens, P("dp", "tp"), P("dp", "tp"), columns, columns, rows),
        out_specs=(tokens, P("dp", "tp"), P("dp", "tp"), P(("dp", "tp"), None)),
        check_vma=False,
    )
```

```python
import functools
import math

import jax
import jax.numpy as jnp
from jax import lax
from jax.experimental import pallas as pl
from jax.experimental.pallas import tpu as pltpu
from jax.sharding import PartitionSpec as P

MESH = pl.DeviceIdType.MESH
F32 = jnp.float32
BF16 = jnp.bfloat16

ROWS = 256
SPLIT = 2
TILE = 256
LAG = (1, 3, 5, 7, 9, 11, 14, 19, 23, 24)
SLOTS = 5
SLOTS2 = 5
PUT = 4
FLIGHT = 4


def nt(a, b):
    return lax.dot_general(a, b, (((1,), (1,)), ((), ())), preferred_element_type=F32)


def tn(a, b):
    return lax.dot_general(a, b, (((0,), (0,)), ((), ())), preferred_element_type=F32)


def kernel(side, x, dy, gate, up, w_gate, w_up, w_down, dx, og, ou, od,
           dyb, gb, ub, dgu, hid, xb, yb, own, own2, far, mid, far2, mid2, relay2,
           w_sem, c_sem, b_sem, send, recv):
    tokens, width = dx.shape
    hidden = od.shape[0]
    half = width // 2
    cu = half // SPLIT
    cw = cu // side
    sub = ROWS // side
    chunks = tokens // ROWS
    units = chunks * SPLIT
    steps = width // TILE

    me = lax.axis_index("tp")
    core = lax.rem(me, 2)
    y = lax.rem(me // 2, side)
    xx = me // (2 * side)
    p1 = xx + core * (y - xx)
    p2 = y + core * (xx - y)

    def device(a, b):
        a, b = lax.rem(a + side, side), lax.rem(b + side, side)
        return ((a + core * (b - a)) * side + b + core * (a - b)) * 2 + core

    right, left = device(p1 + 1, p2), device(p1 - 1, p2)
    right2, left2 = device(p1, p2 + 1), device(p1, p2 - 1)
    partner = me + 1 - 2 * core

    barrier = pltpu.get_barrier_semaphore()
    peers = (partner, right, left, right2, left2)
    for peer in peers:
        pl.semaphore_signal(barrier, inc=1, device_id={"tp": peer}, device_id_type=MESH)

    def load_chunk(r):
        s = lax.rem(r, 2)
        rows = pl.ds(pl.multiple_of(r * ROWS, ROWS), ROWS)
        return (
            pltpu.make_async_copy(dy.at[rows], dyb.at[s], c_sem.at[s, 0]),
            pltpu.make_async_copy(gate.at[rows], gb.at[s], c_sem.at[s, 1]),
            pltpu.make_async_copy(up.at[rows], ub.at[s], c_sem.at[s, 2]),
        )

    def load_tile(j):
        s = lax.rem(j, 2)
        cols = pl.ds(pl.multiple_of(j * TILE, TILE), TILE)
        return (
            pltpu.make_async_copy(x.at[:, cols], xb.at[s], b_sem.at[s, 0]),
            pltpu.make_async_copy(dy.at[:, cols], yb.at[s], b_sem.at[s, 1]),
        )

    def base(u, h):
        return h * half + lax.rem(u, SPLIT) * cu

    load_down = pltpu.make_async_copy(w_down, od, w_sem.at[0])

    def load_block(k, h):
        rows = pl.ds(pl.multiple_of(base(k, core + h * (1 - 2 * core)), cu), cu)
        at = 1 + 2 * (2 * k + h)
        return (
            pltpu.make_async_copy(w_gate.at[rows], og.at[rows], w_sem.at[at]),
            pltpu.make_async_copy(w_up.at[rows], ou.at[rows], w_sem.at[at + 1]),
        )

    load_down.start()
    for c in load_chunk(0):
        c.start()
    for k in range(SPLIT):
        for h in (1, 0):
            for c in load_block(k, h):
                c.start()

    def rows_of(u, first=0, count=ROWS):
        return pl.ds(pl.multiple_of((u // SPLIT) * ROWS + first, math.gcd(count, 64)), count)

    def piece(u, d):
        q = lax.rem(p1 + d, side)
        return q, pl.ds(pl.multiple_of(base(u, core) + q * cw, cw), cw)

    def ship(src, dst, stage, u, to, kind):
        pltpu.make_async_remote_copy(
            src_ref=src, dst_ref=dst, send_sem=send.at[stage, lax.rem(u, FLIGHT) if stage < 5 else 0],
            recv_sem=recv.at[kind, u],
            device_id={"tp": to}, device_id_type=MESH,
        ).start()

    def arrived(ref, kind, u):
        pltpu.make_async_copy(ref, ref, recv.at[kind, u]).wait()

    def amount(rows, cols):
        return dx.at[pl.ds(0, rows), pl.ds(0, cols)]

    def left_with(ref, stage, u):
        pltpu.make_async_copy(ref, ref, send.at[stage, lax.rem(u, FLIGHT)]).wait()

    def s0_hidden(u):
        r = u // SPLIT
        s = lax.rem(r, 2)
        rows = rows_of(u)
        for c in load_chunk(r):
            c.wait()

        @pl.when(r == 0)
        def _():
            load_down.wait()

        dh = nt(dyb[s], od[...])
        g = gb[s].astype(F32)
        v = ub[s].astype(F32)
        sig = jax.nn.sigmoid(g)
        silu = g * sig
        hid[:, pl.ds(pl.multiple_of(r * ROWS, ROWS), ROWS)] = (silu * v).T.astype(BF16)
        dgu[rows, hidden:] = (dh * silu).astype(BF16)
        dgu[rows, :hidden] = (dh * v * (sig + silu * (1.0 - sig))).astype(BF16)

    def s0_term(u, h):
        for k in range(SPLIT):
            @pl.when(u == k)
            def _():
                for c in load_block(k, h):
                    c.wait()

        rows = rows_of(u)
        cols = pl.ds(pl.multiple_of(base(u, core + h * (1 - 2 * core)), cu), cu)
        return nt(dgu[rows, :hidden], og[cols, :]) + nt(dgu[rows, hidden:], ou[cols, :])

    def s0_first(u):
        pl.when(lax.rem(u, SPLIT) == 0)(lambda: s0_hidden(u))
        there = dx.at[rows_of(u), pl.ds(pl.multiple_of(base(u, 1 - core), cu), cu)]
        there[...] = s0_term(u, 1).astype(BF16)
        pl.when(u == 0)(lambda: pl.semaphore_wait(barrier, len(peers)))
        ship(there, there, 0, u, partner, 0)

    def s0_second(u):
        @pl.when((lax.rem(u, SPLIT) == 0) & (u // SPLIT + 1 < chunks))
        def _():
            for c in load_chunk(u // SPLIT + 1):
                c.start()

        own[lax.rem(u, SLOTS)] = s0_term(u, 0)

    hr = ROWS // 2

    def s1(u):
        here = dx.at[rows_of(u), pl.ds(pl.multiple_of(base(u, core), cu), cu)]
        arrived(here, 0, u)
        left_with(amount(ROWS, cu), 0, u)
        mine = own.at[lax.rem(u, SLOTS)]
        upper, lower = rows_of(u, 0, hr), rows_of(u, hr, hr)

        def total(d):
            q, cols = piece(u, d)
            at = pl.ds(pl.multiple_of(q * cw, cw), cw)
            return at, cols, mine[:, at] + dx[rows_of(u), cols].astype(F32)

        at, cols, v = total(side // 2)
        dx[rows_of(u), cols] = v.astype(BF16)
        ship(dx.at[upper, cols], far.at[u, 0], 1, u, left, 1)
        ship(dx.at[lower, cols], far.at[u, 1], 1, u, right, 1)
        at, cols, v = total(1)
        dx[upper, cols] = v[:hr].astype(BF16)
        ship(dx.at[upper, cols], mid.at[u, 0], 1, u, right, 2)
        mine[hr:, at] = v[hr:]
        at, cols, v = total(side - 1)
        dx[lower, cols] = v[hr:].astype(BF16)
        ship(dx.at[lower, cols], mid.at[u, 1], 1, u, left, 2)
        mine[:hr, at] = v[:hr]
        at, cols, v = total(0)
        mine[:, at] = v

    def s2(u):
        arrived(far.at[u], 1, u)
        left_with(amount(2 * ROWS, cw), 1, u)
        mine = own.at[lax.rem(u, SLOTS)]
        upper, lower = rows_of(u, 0, hr), rows_of(u, hr, hr)
        q, cols = piece(u, side - 1)
        at = pl.ds(pl.multiple_of(q * cw, cw), cw)
        dx[upper, cols] = (mine[:hr, at] + far[u, 0].astype(F32)).astype(BF16)
        ship(dx.at[upper, cols], mid.at[u, 2], 2, u, left, 2)
        q, cols = piece(u, 1)
        at = pl.ds(pl.multiple_of(q * cw, cw), cw)
        dx[lower, cols] = (mine[hr:, at] + far[u, 1].astype(F32)).astype(BF16)
        ship(dx.at[lower, cols], mid.at[u, 3], 2, u, right, 2)

    hs = sub // 2

    def part(d):
        return pl.multiple_of(lax.rem(p2 + d, side) * sub, sub)

    def s3(u):
        arrived(mid.at[u], 2, u)
        left_with(amount(ROWS, cw), 2, u)
        q, cols = piece(u, 0)
        at = pl.ds(pl.multiple_of(q * cw, cw), cw)
        mine = own.at[lax.rem(u, SLOTS)]
        keep = own2.at[lax.rem(u, SLOTS2)]
        keep[:hr] = mine[:hr, at] + mid[u, 0].astype(F32) + mid[u, 2].astype(F32)
        keep[hr:] = mine[hr:, at] + mid[u, 1].astype(F32) + mid[u, 3].astype(F32)

        f = part(side // 2)
        dx[rows_of(u, f, sub), cols] = keep[pl.ds(f, sub)].astype(BF16)
        ship(dx.at[rows_of(u, f, hs), cols], far2.at[u, 0], 3, u, left2, 3)
        ship(dx.at[rows_of(u, f + hs, hs), cols], far2.at[u, 1], 3, u, right2, 3)
        f = part(1)
        dx[rows_of(u, f, hs), cols] = keep[pl.ds(f, hs)].astype(BF16)
        ship(dx.at[rows_of(u, f, hs), cols], mid2.at[u, 0], 3, u, right2, 4)
        f = pl.multiple_of(part(side - 1) + hs, hs)
        dx[rows_of(u, f, hs), cols] = keep[pl.ds(f, hs)].astype(BF16)
        ship(dx.at[rows_of(u, f, hs), cols], mid2.at[u, 1], 3, u, left2, 4)

    def s4(u):
        arrived(far2.at[u], 3, u)
        left_with(amount(2 * sub, cw), 3, u)
        keep = own2.at[lax.rem(u, SLOTS2)]
        f = part(side - 1)
        relay2[u, 0] = (keep[pl.ds(f, hs)] + far2[u, 0].astype(F32)).astype(BF16)
        ship(relay2.at[u, 0], mid2.at[u, 2], 4, u, left2, 4)
        f = pl.multiple_of(part(1) + hs, hs)
        relay2[u, 1] = (keep[pl.ds(f, hs)] + far2[u, 1].astype(F32)).astype(BF16)
        ship(relay2.at[u, 1], mid2.at[u, 3], 4, u, right2, 4)

    def s5(u):
        arrived(mid2.at[u], 4, u)
        left_with(amount(sub, cw), 4, u)
        _, cols = piece(u, 0)
        keep = own2.at[lax.rem(u, SLOTS2)]
        f = part(0)
        a = keep[pl.ds(f, hs)] + mid2[u, 0].astype(F32) + mid2[u, 2].astype(F32)
        g = pl.multiple_of(f + hs, hs)
        b = keep[pl.ds(g, hs)] + mid2[u, 1].astype(F32) + mid2[u, 3].astype(F32)
        dx[rows_of(u, f, hs), cols] = a.astype(BF16)
        dx[rows_of(u, g, hs), cols] = b.astype(BF16)
        done = dx.at[rows_of(u, f, sub), cols]
        ship(done, done, 5, u, left2, 5)
        ship(done, done, 5, u, right2, 5)

    def s6(u):
        arrived(amount(2 * sub, cw), 5, u)
        _, cols = piece(u, 0)
        a = dx.at[rows_of(u, part(side - 1), hs), cols]
        b = dx.at[rows_of(u, part(1) + hs, hs), cols]
        ship(a, a, 6, u, right2, 6)
        ship(b, b, 6, u, left2, 6)

    def s7(u):
        arrived(amount(sub, cw), 6, u)
        _, cols = piece(u, 0)
        done = dx.at[rows_of(u), cols]
        ship(done, done, 7, u, left, 7)
        ship(done, done, 7, u, right, 7)
        ship(done, done, 7, u, partner, 9)

    def s8(u):
        arrived(amount(2 * ROWS, cw), 7, u)
        _, lcols = piece(u, side - 1)
        _, rcols = piece(u, 1)
        a = dx.at[rows_of(u, 0, hr), lcols]
        b = dx.at[rows_of(u, hr, hr), rcols]
        ship(a, a, 8, u, right, 8)
        ship(b, b, 8, u, left, 8)
        for cols in (lcols, rcols):
            done = dx.at[rows_of(u), cols]
            ship(done, done, 8, u, partner, 9)

    def s9(u):
        arrived(amount(ROWS, cw), 8, u)
        _, cols = piece(u, side // 2)
        done = dx.at[rows_of(u), cols]
        ship(done, done, 9, u, partner, 9)

    def s10(u):
        arrived(amount(ROWS, cu), 9, u)

    def grads(j):
        s = lax.rem(j, 2)

        @pl.when(j + 1 < steps)
        def _():
            for c in load_tile(j + 1):
                c.start()

        for c in load_tile(j):
            c.wait()
        at = pl.ds(pl.multiple_of(j * TILE, TILE), TILE)
        both = tn(xb[s], dgu[...])
        og[at, :] = both[:, :hidden].astype(BF16)
        ou[at, :] = both[:, hidden:].astype(BF16)
        od[:, at] = jnp.dot(hid[...], yb[s], preferred_element_type=F32).astype(BF16)

    total = units + max(LAG[-1], steps)

    def iteration(i, carry):
        pl.when(i < units)(lambda: s0_first(i))
        for lag, stage in zip(LAG, (s1, s2, s3, s4, s5, s6, s7, s8, s9, s10)):
            pl.when((i >= lag) & (i < units + lag))(functools.partial(stage, i - lag))

        pl.when(i < units)(lambda: s0_second(i))

        @pl.when(i == units // 2)
        def _():
            for c in load_tile(0):
                c.start()

        pl.when((i >= units) & (i < units + steps))(lambda: grads(i - units))
        return carry

    lax.fori_loop(0, total, iteration, 0)

    for stage, share in ((5, 2), (6, 1), (7, 12), (8, 12), (9, 4)):
        ref = dx.at[:, pl.ds(0, share * width // 32)]
        pltpu.make_async_copy(ref, ref, send.at[stage, 0]).wait()


def put_kernel(*refs):
    count = len(refs) // 2
    sems = refs[-1]
    copies = []
    for i, (src, dst) in enumerate(zip(refs[:count], refs[count:2 * count])):
        rows = src.shape[0] // PUT
        for j in range(PUT):
            at = pl.ds(j * rows, rows)
            copies.append(pltpu.make_async_copy(src.at[at], dst.at[at], sems.at[i, j]))
    for c in copies:
        c.start()
    for c in copies:
        c.wait()


def put(found):
    return pl.pallas_call(
        put_kernel,
        out_shape=[pltpu.HBM(a.shape, a.dtype) for a in found],
        in_specs=[pl.BlockSpec(memory_space=pltpu.VMEM)] * len(found),
        out_specs=[pl.BlockSpec(memory_space=pltpu.HBM)] * len(found),
        scratch_shapes=[pltpu.SemaphoreType.DMA((len(found), PUT))],
        compiler_params=pltpu.CompilerParams(vmem_limit_bytes=2**20),
    )(*found)


def solution(mesh):
    side = math.isqrt(mesh.shape["tp"] // 2)

    def step(x, dy, gate, up, w_gate, w_up, w_down):
        tokens, width = x.shape
        hidden = gate.shape[1]
        units = tokens // ROWS * SPLIT
        cu = width // 2 // SPLIT
        cw = cu // side
        sub = ROWS // side
        out = [pltpu.VMEM(a.shape, a.dtype) for a in (x, w_gate, w_up, w_down)]
        dma = pltpu.SemaphoreType.DMA
        found = pl.pallas_call(
            functools.partial(kernel, side),
            out_shape=out,
            in_specs=[pl.BlockSpec(memory_space=pl.ANY)] * 7,
            out_specs=[pl.BlockSpec(memory_space=pltpu.VMEM)] * 4,
            scratch_shapes=[
                pltpu.VMEM((2, ROWS, width), BF16),
                pltpu.VMEM((2, ROWS, hidden), BF16),
                pltpu.VMEM((2, ROWS, hidden), BF16),
                pltpu.VMEM((tokens, 2 * hidden), BF16),
                pltpu.VMEM((hidden, tokens), BF16),
                pltpu.VMEM((2, tokens, TILE), BF16),
                pltpu.VMEM((2, tokens, TILE), BF16),
                pltpu.VMEM((SLOTS, ROWS, cu), F32),
                pltpu.VMEM((SLOTS2, ROWS, cw), F32),
                pltpu.VMEM((units, 2, ROWS // 2, cw), BF16),
                pltpu.VMEM((units, 4, ROWS // 2, cw), BF16),
                pltpu.VMEM((units, 2, sub // 2, cw), BF16),
                pltpu.VMEM((units, 4, sub // 2, cw), BF16),
                pltpu.VMEM((units, 2, sub // 2, cw), BF16),
                dma((1 + 4 * SPLIT,)),
                dma((2, 3)),
                dma((2, 2)),
                dma((10, FLIGHT)),
                dma((10, units)),
            ],
            compiler_params=pltpu.CompilerParams(
                collective_id=0, has_side_effects=True, vmem_limit_bytes=34 * 2**20,
            ),
        )(x, dy, gate, up, w_gate, w_up, w_down)
        return tuple(put(found))

    tokens, columns, rows = P("dp", None), P(None, "tp"), P("tp", None)
    return jax.shard_map(
        step,
        mesh=mesh,
        in_specs=(tokens, tokens, P("dp", "tp"), P("dp", "tp"), columns, columns, rows),
        out_specs=(tokens, P("dp", "tp"), P("dp", "tp"), P(("dp", "tp"), None)),
        check_vma=False,
    )
```

```python
import functools
import math

import jax
import jax.numpy as jnp
from jax import lax
from jax.experimental import pallas as pl
from jax.experimental.pallas import tpu as pltpu
from jax.sharding import PartitionSpec as P

MESH = pl.DeviceIdType.MESH
F32 = jnp.float32
BF16 = jnp.bfloat16

ROWS = 256
SPLIT = 2
TILE = 256
LAG = (1, 3, 6, 8, 10, 12, 14, 18, 23, 24)
SLOTS = 6
SLOTS2 = 5
PUT = 4
FLIGHT = 4
VMEM = 35


def nt(a, b):
    return lax.dot_general(a, b, (((1,), (1,)), ((), ())), preferred_element_type=F32)


def tn(a, b):
    return lax.dot_general(a, b, (((0,), (0,)), ((), ())), preferred_element_type=F32)


def kernel(side, x, dy, gate, up, w_gate, w_up, w_down, dx, og, ou, od,
           dyb, gb, ub, dgu, hid, xb, yb, own, own2, far, mid, far2, mid2, relay2,
           w_sem, c_sem, b_sem, send, recv):
    tokens, width = dx.shape
    hidden = od.shape[0]
    half = width // 2
    cu = half // SPLIT
    cw = cu // side
    sub = ROWS // side
    chunks = tokens // ROWS
    units = chunks * SPLIT
    steps = width // TILE

    me = lax.axis_index("tp")
    core = lax.rem(me, 2)
    y = lax.rem(me // 2, side)
    xx = me // (2 * side)
    p1 = xx + core * (y - xx)
    p2 = y + core * (xx - y)

    def device(a, b):
        a, b = lax.rem(a + side, side), lax.rem(b + side, side)
        return ((a + core * (b - a)) * side + b + core * (a - b)) * 2 + core

    right, left = device(p1 + 1, p2), device(p1 - 1, p2)
    right2, left2 = device(p1, p2 + 1), device(p1, p2 - 1)
    partner = me + 1 - 2 * core

    barrier = pltpu.get_barrier_semaphore()
    peers = (partner, right, left, right2, left2)
    for peer in peers:
        pl.semaphore_signal(barrier, inc=1, device_id={"tp": peer}, device_id_type=MESH)

    def load_chunk(r):
        s = lax.rem(r, 2)
        rows = pl.ds(pl.multiple_of(r * ROWS, ROWS), ROWS)
        return (
            pltpu.make_async_copy(dy.at[rows], dyb.at[s], c_sem.at[s, 0]),
            pltpu.make_async_copy(gate.at[rows], gb.at[s], c_sem.at[s, 1]),
            pltpu.make_async_copy(up.at[rows], ub.at[s], c_sem.at[s, 2]),
        )

    def load_tile(j):
        s = lax.rem(j, 2)
        cols = pl.ds(pl.multiple_of(j * TILE, TILE), TILE)
        return (
            pltpu.make_async_copy(x.at[:, cols], xb.at[s], b_sem.at[s, 0]),
            pltpu.make_async_copy(dy.at[:, cols], yb.at[s], b_sem.at[s, 1]),
        )

    def base(u, h):
        return h * half + lax.rem(u, SPLIT) * cu

    load_down = pltpu.make_async_copy(w_down, od, w_sem.at[0])

    def load_block(k, h):
        rows = pl.ds(pl.multiple_of(base(k, core + h * (1 - 2 * core)), cu), cu)
        at = 1 + 2 * (2 * k + h)
        return (
            pltpu.make_async_copy(w_gate.at[rows], og.at[rows], w_sem.at[at]),
            pltpu.make_async_copy(w_up.at[rows], ou.at[rows], w_sem.at[at + 1]),
        )

    load_down.start()
    for c in load_chunk(0):
        c.start()
    def start_blocks(k):
        for h in (1, 0):
            for c in load_block(k, h):
                c.start()

    def rows_of(u, first=0, count=ROWS):
        return pl.ds(pl.multiple_of((u // SPLIT) * ROWS + first, math.gcd(count, 64)), count)

    def piece(u, d):
        q = lax.rem(p1 + d, side)
        return q, pl.ds(pl.multiple_of(base(u, core) + q * cw, cw), cw)

    def ship(src, dst, stage, u, to, kind):
        pltpu.make_async_remote_copy(
            src_ref=src, dst_ref=dst, send_sem=send.at[stage, lax.rem(u, FLIGHT) if stage < 5 else 0],
            recv_sem=recv.at[kind, u],
            device_id={"tp": to}, device_id_type=MESH,
        ).start()

    def arrived(ref, kind, u):
        pltpu.make_async_copy(ref, ref, recv.at[kind, u]).wait()

    def amount(rows, cols):
        return dx.at[pl.ds(0, rows), pl.ds(0, cols)]

    def left_with(ref, stage, u):
        pltpu.make_async_copy(ref, ref, send.at[stage, lax.rem(u, FLIGHT)]).wait()

    def s0_hidden(u):
        r = u // SPLIT
        s = lax.rem(r, 2)
        rows = rows_of(u)
        for c in load_chunk(r):
            c.wait()

        @pl.when(r == 0)
        def _():
            start_blocks(0)
            load_down.wait()
            for k in range(1, SPLIT):
                start_blocks(k)

        dh = nt(dyb[s], od[...])
        g = gb[s].astype(F32)
        v = ub[s].astype(F32)
        sig = jax.nn.sigmoid(g)
        silu = g * sig
        hid[:, pl.ds(pl.multiple_of(r * ROWS, ROWS), ROWS)] = (silu * v).T.astype(BF16)
        dgu[rows, hidden:] = (dh * silu).astype(BF16)
        dgu[rows, :hidden] = (dh * v * (sig + silu * (1.0 - sig))).astype(BF16)

    def s0_term(u, h):
        for k in range(SPLIT):
            @pl.when(u == k)
            def _():
                for c in load_block(k, h):
                    c.wait()

        rows = rows_of(u)
        cols = pl.ds(pl.multiple_of(base(u, core + h * (1 - 2 * core)), cu), cu)
        return nt(dgu[rows, :hidden], og[cols, :]) + nt(dgu[rows, hidden:], ou[cols, :])

    def s0_first(u):
        pl.when(lax.rem(u, SPLIT) == 0)(lambda: s0_hidden(u))
        there = dx.at[rows_of(u), pl.ds(pl.multiple_of(base(u, 1 - core), cu), cu)]
        there[...] = s0_term(u, 1).astype(BF16)
        pl.when(u == 0)(lambda: pl.semaphore_wait(barrier, len(peers)))
        ship(there, there, 0, u, partner, 0)

    def s0_second(u):
        @pl.when((lax.rem(u, SPLIT) == 0) & (u // SPLIT + 1 < chunks))
        def _():
            for c in load_chunk(u // SPLIT + 1):
                c.start()

        own[lax.rem(u, SLOTS)] = s0_term(u, 0)

    hr = ROWS // 2

    def s1(u):
        here = dx.at[rows_of(u), pl.ds(pl.multiple_of(base(u, core), cu), cu)]
        arrived(here, 0, u)
        left_with(amount(ROWS, cu), 0, u)
        mine = own.at[lax.rem(u, SLOTS)]
        upper, lower = rows_of(u, 0, hr), rows_of(u, hr, hr)

        def total(d):
            q, cols = piece(u, d)
            at = pl.ds(pl.multiple_of(q * cw, cw), cw)
            return at, cols, mine[:, at] + dx[rows_of(u), cols].astype(F32)

        at, cols, v = total(side // 2)
        dx[rows_of(u), cols] = v.astype(BF16)
        ship(dx.at[upper, cols], far.at[u, 0], 1, u, left, 1)
        ship(dx.at[lower, cols], far.at[u, 1], 1, u, right, 1)
        at, cols, v = total(1)
        dx[upper, cols] = v[:hr].astype(BF16)
        ship(dx.at[upper, cols], mid.at[u, 0], 1, u, right, 2)
        mine[hr:, at] = v[hr:]
        at, cols, v = total(side - 1)
        dx[lower, cols] = v[hr:].astype(BF16)
        ship(dx.at[lower, cols], mid.at[u, 1], 1, u, left, 2)
        mine[:hr, at] = v[:hr]
        at, cols, v = total(0)
        mine[:, at] = v

    def s2(u):
        arrived(far.at[u], 1, u)
        left_with(amount(2 * ROWS, cw), 1, u)
        mine = own.at[lax.rem(u, SLOTS)]
        upper, lower = rows_of(u, 0, hr), rows_of(u, hr, hr)
        q, cols = piece(u, side - 1)
        at = pl.ds(pl.multiple_of(q * cw, cw), cw)
        dx[upper, cols] = (mine[:hr, at] + far[u, 0].astype(F32)).astype(BF16)
        ship(dx.at[upper, cols], mid.at[u, 2], 2, u, left, 2)
        q, cols = piece(u, 1)
        at = pl.ds(pl.multiple_of(q * cw, cw), cw)
        dx[lower, cols] = (mine[hr:, at] + far[u, 1].astype(F32)).astype(BF16)
        ship(dx.at[lower, cols], mid.at[u, 3], 2, u, right, 2)

    hs = sub // 2

    def part(d):
        return pl.multiple_of(lax.rem(p2 + d, side) * sub, sub)

    def s3(u):
        arrived(mid.at[u], 2, u)
        left_with(amount(ROWS, cw), 2, u)
        q, cols = piece(u, 0)
        at = pl.ds(pl.multiple_of(q * cw, cw), cw)
        mine = own.at[lax.rem(u, SLOTS)]
        keep = own2.at[lax.rem(u, SLOTS2)]
        keep[:hr] = mine[:hr, at] + mid[u, 0].astype(F32) + mid[u, 2].astype(F32)
        keep[hr:] = mine[hr:, at] + mid[u, 1].astype(F32) + mid[u, 3].astype(F32)

        f = part(side // 2)
        dx[rows_of(u, f, sub), cols] = keep[pl.ds(f, sub)].astype(BF16)
        ship(dx.at[rows_of(u, f, hs), cols], far2.at[u, 0], 3, u, left2, 3)
        ship(dx.at[rows_of(u, f + hs, hs), cols], far2.at[u, 1], 3, u, right2, 3)
        f = part(1)
        dx[rows_of(u, f, hs), cols] = keep[pl.ds(f, hs)].astype(BF16)
        ship(dx.at[rows_of(u, f, hs), cols], mid2.at[u, 0], 3, u, right2, 4)
        f = pl.multiple_of(part(side - 1) + hs, hs)
        dx[rows_of(u, f, hs), cols] = keep[pl.ds(f, hs)].astype(BF16)
        ship(dx.at[rows_of(u, f, hs), cols], mid2.at[u, 1], 3, u, left2, 4)

    def s4(u):
        arrived(far2.at[u], 3, u)
        left_with(amount(2 * sub, cw), 3, u)
        keep = own2.at[lax.rem(u, SLOTS2)]
        f = part(side - 1)
        relay2[u, 0] = (keep[pl.ds(f, hs)] + far2[u, 0].astype(F32)).astype(BF16)
        ship(relay2.at[u, 0], mid2.at[u, 2], 4, u, left2, 4)
        f = pl.multiple_of(part(1) + hs, hs)
        relay2[u, 1] = (keep[pl.ds(f, hs)] + far2[u, 1].astype(F32)).astype(BF16)
        ship(relay2.at[u, 1], mid2.at[u, 3], 4, u, right2, 4)

    def s5(u):
        arrived(mid2.at[u], 4, u)
        left_with(amount(sub, cw), 4, u)
        _, cols = piece(u, 0)
        keep = own2.at[lax.rem(u, SLOTS2)]
        f = part(0)
        a = keep[pl.ds(f, hs)] + mid2[u, 0].astype(F32) + mid2[u, 2].astype(F32)
        g = pl.multiple_of(f + hs, hs)
        b = keep[pl.ds(g, hs)] + mid2[u, 1].astype(F32) + mid2[u, 3].astype(F32)
        dx[rows_of(u, f, hs), cols] = a.astype(BF16)
        dx[rows_of(u, g, hs), cols] = b.astype(BF16)
        done = dx.at[rows_of(u, f, sub), cols]
        ship(done, done, 5, u, left2, 5)
        ship(done, done, 5, u, right2, 5)

    def s6(u):
        arrived(amount(2 * sub, cw), 5, u)
        _, cols = piece(u, 0)
        a = dx.at[rows_of(u, part(side - 1), hs), cols]
        b = dx.at[rows_of(u, part(1) + hs, hs), cols]
        ship(a, a, 6, u, right2, 6)
        ship(b, b, 6, u, left2, 6)

    def s7(u):
        arrived(amount(sub, cw), 6, u)
        _, cols = piece(u, 0)
        done = dx.at[rows_of(u), cols]
        ship(done, done, 7, u, left, 7)
        ship(done, done, 7, u, right, 7)
        ship(done, done, 7, u, partner, 9)

    def s8(u):
        arrived(amount(2 * ROWS, cw), 7, u)
        _, lcols = piece(u, side - 1)
        _, rcols = piece(u, 1)
        a = dx.at[rows_of(u, 0, hr), lcols]
        b = dx.at[rows_of(u, hr, hr), rcols]
        ship(a, a, 8, u, right, 8)
        ship(b, b, 8, u, left, 8)
        for cols in (lcols, rcols):
            done = dx.at[rows_of(u), cols]
            ship(done, done, 8, u, partner, 9)

    def s9(u):
        arrived(amount(ROWS, cw), 8, u)
        _, cols = piece(u, side // 2)
        done = dx.at[rows_of(u), cols]
        ship(done, done, 9, u, partner, 9)

    def s10(u):
        arrived(amount(ROWS, cu), 9, u)

    def grads(j):
        s = lax.rem(j, 2)

        @pl.when(j + 1 < steps)
        def _():
            for c in load_tile(j + 1):
                c.start()

        for c in load_tile(j):
            c.wait()
        at = pl.ds(pl.multiple_of(j * TILE, TILE), TILE)
        both = tn(xb[s], dgu[...])
        og[at, :] = both[:, :hidden].astype(BF16)
        ou[at, :] = both[:, hidden:].astype(BF16)
        od[:, at] = jnp.dot(hid[...], yb[s], preferred_element_type=F32).astype(BF16)

    total = units + max(LAG[-1], steps)

    def iteration(i, carry):
        pl.when(i < units)(lambda: s0_first(i))
        def link_step(lag, stage):
            pl.when((i >= lag) & (i < units + lag))(functools.partial(stage, i - lag))

        for lag, stage in zip(LAG[:3], (s1, s2, s3)):
            link_step(lag, stage)
        pl.when(i < units)(lambda: s0_second(i))
        for lag, stage in zip(LAG[3:], (s4, s5, s6, s7, s8, s9, s10)):
            link_step(lag, stage)

        @pl.when(i == units // 2)
        def _():
            for c in load_tile(0):
                c.start()

        pl.when((i >= units) & (i < units + steps))(lambda: grads(i - units))
        return carry

    lax.fori_loop(0, total, iteration, 0)

    for stage, share in ((5, 2), (6, 1), (7, 12), (8, 12), (9, 4)):
        ref = dx.at[:, pl.ds(0, share * width // 32)]
        pltpu.make_async_copy(ref, ref, send.at[stage, 0]).wait()


def put_kernel(*refs):
    count = len(refs) // 2
    sems = refs[-1]
    copies = []
    for i, (src, dst) in enumerate(zip(refs[:count], refs[count:2 * count])):
        rows = src.shape[0] // PUT
        for j in range(PUT):
            at = pl.ds(j * rows, rows)
            copies.append(pltpu.make_async_copy(src.at[at], dst.at[at], sems.at[i, j]))
    for c in copies:
        c.start()
    for c in copies:
        c.wait()


def put(found):
    return pl.pallas_call(
        put_kernel,
        out_shape=[pltpu.HBM(a.shape, a.dtype) for a in found],
        in_specs=[pl.BlockSpec(memory_space=pltpu.VMEM)] * len(found),
        out_specs=[pl.BlockSpec(memory_space=pltpu.HBM)] * len(found),
        scratch_shapes=[pltpu.SemaphoreType.DMA((len(found), PUT))],
        compiler_params=pltpu.CompilerParams(vmem_limit_bytes=2**20),
    )(*found)


def solution(mesh):
    side = math.isqrt(mesh.shape["tp"] // 2)

    def step(x, dy, gate, up, w_gate, w_up, w_down):
        tokens, width = x.shape
        hidden = gate.shape[1]
        units = tokens // ROWS * SPLIT
        cu = width // 2 // SPLIT
        cw = cu // side
        sub = ROWS // side
        out = [pltpu.VMEM(a.shape, a.dtype) for a in (x, w_gate, w_up, w_down)]
        dma = pltpu.SemaphoreType.DMA
        found = pl.pallas_call(
            functools.partial(kernel, side),
            out_shape=out,
            in_specs=[pl.BlockSpec(memory_space=pl.ANY)] * 7,
            out_specs=[pl.BlockSpec(memory_space=pltpu.VMEM)] * 4,
            scratch_shapes=[
                pltpu.VMEM((2, ROWS, width), BF16),
                pltpu.VMEM((2, ROWS, hidden), BF16),
                pltpu.VMEM((2, ROWS, hidden), BF16),
                pltpu.VMEM((tokens, 2 * hidden), BF16),
                pltpu.VMEM((hidden, tokens), BF16),
                pltpu.VMEM((2, tokens, TILE), BF16),
                pltpu.VMEM((2, tokens, TILE), BF16),
                pltpu.VMEM((SLOTS, ROWS, cu), F32),
                pltpu.VMEM((SLOTS2, ROWS, cw), F32),
                pltpu.VMEM((units, 2, ROWS // 2, cw), BF16),
                pltpu.VMEM((units, 4, ROWS // 2, cw), BF16),
                pltpu.VMEM((units, 2, sub // 2, cw), BF16),
                pltpu.VMEM((units, 4, sub // 2, cw), BF16),
                pltpu.VMEM((units, 2, sub // 2, cw), BF16),
                dma((1 + 4 * SPLIT,)),
                dma((2, 3)),
                dma((2, 2)),
                dma((10, FLIGHT)),
                dma((10, units)),
            ],
            compiler_params=pltpu.CompilerParams(
                collective_id=0, has_side_effects=True, vmem_limit_bytes=VMEM * 2**20,
            ),
        )(x, dy, gate, up, w_gate, w_up, w_down)
        return tuple(put(found))

    tokens, columns, rows = P("dp", None), P(None, "tp"), P("tp", None)
    return jax.shard_map(
        step,
        mesh=mesh,
        in_specs=(tokens, tokens, P("dp", "tp"), P("dp", "tp"), columns, columns, rows),
        out_specs=(tokens, P("dp", "tp"), P("dp", "tp"), P(("dp", "tp"), None)),
        check_vma=False,
    )
```

```python
import functools
import math

import jax
import jax.numpy as jnp
from jax import lax
from jax.experimental import pallas as pl
from jax.experimental.pallas import tpu as pltpu
from jax.sharding import PartitionSpec as P

MESH = pl.DeviceIdType.MESH
F32 = jnp.float32
BF16 = jnp.bfloat16

ROWS = 256
SPLIT = 2
TILE = 256
LAG = (1, 3, 6, 8, 10, 12, 14, 18, 23, 24)
SLOTS = 6
SLOTS2 = 5
PUT = 4
FLIGHT = 4
VMEM = 35


def nt(a, b):
    return lax.dot_general(a, b, (((1,), (1,)), ((), ())), preferred_element_type=F32)


def tn(a, b):
    return lax.dot_general(a, b, (((0,), (0,)), ((), ())), preferred_element_type=F32)


def kernel(side, x, dy, gate, up, w_gate, w_up, w_down, dx, og, ou, od,
           dyb, gb, ub, dgu, hid, xb, yb, own, own2, far, mid, far2, mid2, relay2,
           w_sem, c_sem, b_sem, send, recv):
    tokens, width = dx.shape
    hidden = od.shape[0]
    half = width // 2
    cu = half // SPLIT
    cw = cu // side
    sub = ROWS // side
    chunks = tokens // ROWS
    units = chunks * SPLIT
    steps = width // TILE

    me = lax.axis_index("tp")
    core = lax.rem(me, 2)
    y = lax.rem(me // 2, side)
    xx = me // (2 * side)
    p1 = xx + core * (y - xx)
    p2 = y + core * (xx - y)

    def device(a, b):
        a, b = lax.rem(a + side, side), lax.rem(b + side, side)
        return ((a + core * (b - a)) * side + b + core * (a - b)) * 2 + core

    right, left = device(p1 + 1, p2), device(p1 - 1, p2)
    right2, left2 = device(p1, p2 + 1), device(p1, p2 - 1)
    partner = me + 1 - 2 * core

    barrier = pltpu.get_barrier_semaphore()
    peers = (partner, right, left, right2, left2)
    for peer in peers:
        pl.semaphore_signal(barrier, inc=1, device_id={"tp": peer}, device_id_type=MESH)

    def load_chunk(r):
        s = lax.rem(r, 2)
        rows = pl.ds(pl.multiple_of(r * ROWS, ROWS), ROWS)
        return (
            pltpu.make_async_copy(dy.at[rows], dyb.at[s], c_sem.at[s, 0]),
            pltpu.make_async_copy(gate.at[rows], gb.at[s], c_sem.at[s, 1]),
            pltpu.make_async_copy(up.at[rows], ub.at[s], c_sem.at[s, 2]),
        )

    def load_tile(j):
        s = lax.rem(j, 2)
        cols = pl.ds(pl.multiple_of(j * TILE, TILE), TILE)
        return (
            pltpu.make_async_copy(x.at[:, cols], xb.at[s], b_sem.at[s, 0]),
            pltpu.make_async_copy(dy.at[:, cols], yb.at[s], b_sem.at[s, 1]),
        )

    def base(u, h):
        return h * half + lax.rem(u, SPLIT) * cu

    load_down = pltpu.make_async_copy(w_down, od, w_sem.at[0])

    def load_block(k, h):
        rows = pl.ds(pl.multiple_of(base(k, core + h * (1 - 2 * core)), cu), cu)
        at = 1 + 2 * (2 * k + h)
        return (
            pltpu.make_async_copy(w_gate.at[rows], og.at[rows], w_sem.at[at]),
            pltpu.make_async_copy(w_up.at[rows], ou.at[rows], w_sem.at[at + 1]),
        )

    for c in load_chunk(0):
        c.start()
    load_down.start()
    def start_blocks(k):
        for h in (1, 0):
            for c in load_block(k, h):
                c.start()

    def rows_of(u, first=0, count=ROWS):
        return pl.ds(pl.multiple_of((u // SPLIT) * ROWS + first, math.gcd(count, 64)), count)

    def piece(u, d):
        q = lax.rem(p1 + d, side)
        return q, pl.ds(pl.multiple_of(base(u, core) + q * cw, cw), cw)

    def ship(src, dst, stage, u, to, kind):
        pltpu.make_async_remote_copy(
            src_ref=src, dst_ref=dst, send_sem=send.at[stage, lax.rem(u, FLIGHT) if stage < 5 else 0],
            recv_sem=recv.at[kind, u],
            device_id={"tp": to}, device_id_type=MESH,
        ).start()

    def arrived(ref, kind, u):
        pltpu.make_async_copy(ref, ref, recv.at[kind, u]).wait()

    def amount(rows, cols):
        return dx.at[pl.ds(0, rows), pl.ds(0, cols)]

    def left_with(ref, stage, u):
        pltpu.make_async_copy(ref, ref, send.at[stage, lax.rem(u, FLIGHT)]).wait()

    def s0_hidden(u):
        r = u // SPLIT
        s = lax.rem(r, 2)
        rows = rows_of(u)
        for c in load_chunk(r):
            c.wait()

        @pl.when(r == 0)
        def _():
            start_blocks(0)
            load_down.wait()
            for k in range(1, SPLIT):
                start_blocks(k)

        dh = nt(dyb[s], od[...])
        g = gb[s].astype(F32)
        v = ub[s].astype(F32)
        sig = jax.nn.sigmoid(g)
        silu = g * sig
        hid[:, pl.ds(pl.multiple_of(r * ROWS, ROWS), ROWS)] = (silu * v).T.astype(BF16)
        dgu[rows, hidden:] = (dh * silu).astype(BF16)
        dgu[rows, :hidden] = (dh * v * (sig + silu * (1.0 - sig))).astype(BF16)

    def s0_term(u, h):
        for k in range(SPLIT):
            @pl.when(u == k)
            def _():
                for c in load_block(k, h):
                    c.wait()

        rows = rows_of(u)
        cols = pl.ds(pl.multiple_of(base(u, core + h * (1 - 2 * core)), cu), cu)
        return nt(dgu[rows, :hidden], og[cols, :]) + nt(dgu[rows, hidden:], ou[cols, :])

    def s0_first(u):
        pl.when(lax.rem(u, SPLIT) == 0)(lambda: s0_hidden(u))
        there = dx.at[rows_of(u), pl.ds(pl.multiple_of(base(u, 1 - core), cu), cu)]
        there[...] = s0_term(u, 1).astype(BF16)
        pl.when(u == 0)(lambda: pl.semaphore_wait(barrier, len(peers)))
        ship(there, there, 0, u, partner, 0)

    def s0_second(u):
        @pl.when((lax.rem(u, SPLIT) == 0) & (u // SPLIT + 1 < chunks))
        def _():
            for c in load_chunk(u // SPLIT + 1):
                c.start()

        own[lax.rem(u, SLOTS)] = s0_term(u, 0)

    hr = ROWS // 2

    def s1(u):
        here = dx.at[rows_of(u), pl.ds(pl.multiple_of(base(u, core), cu), cu)]
        arrived(here, 0, u)
        left_with(amount(ROWS, cu), 0, u)
        mine = own.at[lax.rem(u, SLOTS)]
        upper, lower = rows_of(u, 0, hr), rows_of(u, hr, hr)

        def total(d):
            q, cols = piece(u, d)
            at = pl.ds(pl.multiple_of(q * cw, cw), cw)
            return at, cols, mine[:, at] + dx[rows_of(u), cols].astype(F32)

        at, cols, v = total(side // 2)
        dx[rows_of(u), cols] = v.astype(BF16)
        ship(dx.at[upper, cols], far.at[u, 0], 1, u, left, 1)
        ship(dx.at[lower, cols], far.at[u, 1], 1, u, right, 1)
        at, cols, v = total(1)
        dx[upper, cols] = v[:hr].astype(BF16)
        ship(dx.at[upper, cols], mid.at[u, 0], 1, u, right, 2)
        mine[hr:, at] = v[hr:]
        at, cols, v = total(side - 1)
        dx[lower, cols] = v[hr:].astype(BF16)
        ship(dx.at[lower, cols], mid.at[u, 1], 1, u, left, 2)
        mine[:hr, at] = v[:hr]
        at, cols, v = total(0)
        mine[:, at] = v

    def s2(u):
        arrived(far.at[u], 1, u)
        left_with(amount(2 * ROWS, cw), 1, u)
        mine = own.at[lax.rem(u, SLOTS)]
        upper, lower = rows_of(u, 0, hr), rows_of(u, hr, hr)
        q, cols = piece(u, side - 1)
        at = pl.ds(pl.multiple_of(q * cw, cw), cw)
        dx[upper, cols] = (mine[:hr, at] + far[u, 0].astype(F32)).astype(BF16)
        ship(dx.at[upper, cols], mid.at[u, 2], 2, u, left, 2)
        q, cols = piece(u, 1)
        at = pl.ds(pl.multiple_of(q * cw, cw), cw)
        dx[lower, cols] = (mine[hr:, at] + far[u, 1].astype(F32)).astype(BF16)
        ship(dx.at[lower, cols], mid.at[u, 3], 2, u, right, 2)

    hs = sub // 2

    def part(d):
        return pl.multiple_of(lax.rem(p2 + d, side) * sub, sub)

    def s3(u):
        arrived(mid.at[u], 2, u)
        left_with(amount(ROWS, cw), 2, u)
        q, cols = piece(u, 0)
        at = pl.ds(pl.multiple_of(q * cw, cw), cw)
        mine = own.at[lax.rem(u, SLOTS)]
        keep = own2.at[lax.rem(u, SLOTS2)]
        keep[:hr] = mine[:hr, at] + mid[u, 0].astype(F32) + mid[u, 2].astype(F32)
        keep[hr:] = mine[hr:, at] + mid[u, 1].astype(F32) + mid[u, 3].astype(F32)

        f = part(side // 2)
        dx[rows_of(u, f, sub), cols] = keep[pl.ds(f, sub)].astype(BF16)
        ship(dx.at[rows_of(u, f, hs), cols], far2.at[u, 0], 3, u, left2, 3)
        ship(dx.at[rows_of(u, f + hs, hs), cols], far2.at[u, 1], 3, u, right2, 3)
        f = part(1)
        dx[rows_of(u, f, hs), cols] = keep[pl.ds(f, hs)].astype(BF16)
        ship(dx.at[rows_of(u, f, hs), cols], mid2.at[u, 0], 3, u, right2, 4)
        f = pl.multiple_of(part(side - 1) + hs, hs)
        dx[rows_of(u, f, hs), cols] = keep[pl.ds(f, hs)].astype(BF16)
        ship(dx.at[rows_of(u, f, hs), cols], mid2.at[u, 1], 3, u, left2, 4)

    def s4(u):
        arrived(far2.at[u], 3, u)
        left_with(amount(2 * sub, cw), 3, u)
        keep = own2.at[lax.rem(u, SLOTS2)]
        f = part(side - 1)
        relay2[u, 0] = (keep[pl.ds(f, hs)] + far2[u, 0].astype(F32)).astype(BF16)
        ship(relay2.at[u, 0], mid2.at[u, 2], 4, u, left2, 4)
        f = pl.multiple_of(part(1) + hs, hs)
        relay2[u, 1] = (keep[pl.ds(f, hs)] + far2[u, 1].astype(F32)).astype(BF16)
        ship(relay2.at[u, 1], mid2.at[u, 3], 4, u, right2, 4)

    def s5(u):
        arrived(mid2.at[u], 4, u)
        left_with(amount(sub, cw), 4, u)
        _, cols = piece(u, 0)
        keep = own2.at[lax.rem(u, SLOTS2)]
        f = part(0)
        a = keep[pl.ds(f, hs)] + mid2[u, 0].astype(F32) + mid2[u, 2].astype(F32)
        g = pl.multiple_of(f + hs, hs)
        b = keep[pl.ds(g, hs)] + mid2[u, 1].astype(F32) + mid2[u, 3].astype(F32)
        dx[rows_of(u, f, hs), cols] = a.astype(BF16)
        dx[rows_of(u, g, hs), cols] = b.astype(BF16)
        done = dx.at[rows_of(u, f, sub), cols]
        ship(done, done, 5, u, left2, 5)
        ship(done, done, 5, u, right2, 5)

    def s6(u):
        arrived(amount(2 * sub, cw), 5, u)
        _, cols = piece(u, 0)
        a = dx.at[rows_of(u, part(side - 1), hs), cols]
        b = dx.at[rows_of(u, part(1) + hs, hs), cols]
        ship(a, a, 6, u, right2, 6)
        ship(b, b, 6, u, left2, 6)

    def s7(u):
        arrived(amount(sub, cw), 6, u)
        _, cols = piece(u, 0)
        done = dx.at[rows_of(u), cols]
        ship(done, done, 7, u, left, 7)
        ship(done, done, 7, u, right, 7)
        ship(done, done, 7, u, partner, 9)

    def s8(u):
        arrived(amount(2 * ROWS, cw), 7, u)
        _, lcols = piece(u, side - 1)
        _, rcols = piece(u, 1)
        a = dx.at[rows_of(u, 0, hr), lcols]
        b = dx.at[rows_of(u, hr, hr), rcols]
        ship(a, a, 8, u, right, 8)
        ship(b, b, 8, u, left, 8)
        for cols in (lcols, rcols):
            done = dx.at[rows_of(u), cols]
            ship(done, done, 8, u, partner, 9)

    def s9(u):
        arrived(amount(ROWS, cw), 8, u)
        _, cols = piece(u, side // 2)
        done = dx.at[rows_of(u), cols]
        ship(done, done, 9, u, partner, 9)

    def s10(u):
        arrived(amount(ROWS, cu), 9, u)

    def grads(j):
        s = lax.rem(j, 2)

        @pl.when(j + 1 < steps)
        def _():
            for c in load_tile(j + 1):
                c.start()

        for c in load_tile(j):
            c.wait()
        at = pl.ds(pl.multiple_of(j * TILE, TILE), TILE)
        both = tn(xb[s], dgu[...])
        og[at, :] = both[:, :hidden].astype(BF16)
        ou[at, :] = both[:, hidden:].astype(BF16)
        od[:, at] = jnp.dot(hid[...], yb[s], preferred_element_type=F32).astype(BF16)

    total = units + max(LAG[-1], steps)

    def iteration(i, carry):
        pl.when(i < units)(lambda: s0_first(i))
        def link_step(lag, stage):
            pl.when((i >= lag) & (i < units + lag))(functools.partial(stage, i - lag))

        for lag, stage in zip(LAG[:3], (s1, s2, s3)):
            link_step(lag, stage)
        pl.when(i < units)(lambda: s0_second(i))
        for lag, stage in zip(LAG[3:], (s4, s5, s6, s7, s8, s9, s10)):
            link_step(lag, stage)

        @pl.when(i == units // 2)
        def _():
            for c in load_tile(0):
                c.start()

        pl.when((i >= units) & (i < units + steps))(lambda: grads(i - units))
        return carry

    lax.fori_loop(0, total, iteration, 0)

    for stage, share in ((5, 2), (6, 1), (7, 12), (8, 12), (9, 4)):
        ref = dx.at[:, pl.ds(0, share * width // 32)]
        pltpu.make_async_copy(ref, ref, send.at[stage, 0]).wait()


def put_kernel(*refs):
    count = len(refs) // 2
    sems = refs[-1]
    copies = []
    for i, (src, dst) in enumerate(zip(refs[:count], refs[count:2 * count])):
        rows = src.shape[0] // PUT
        for j in range(PUT):
            at = pl.ds(j * rows, rows)
            copies.append(pltpu.make_async_copy(src.at[at], dst.at[at], sems.at[i, j]))
    for c in copies:
        c.start()
    for c in copies:
        c.wait()


def put(found):
    return pl.pallas_call(
        put_kernel,
        out_shape=[pltpu.HBM(a.shape, a.dtype) for a in found],
        in_specs=[pl.BlockSpec(memory_space=pltpu.VMEM)] * len(found),
        out_specs=[pl.BlockSpec(memory_space=pltpu.HBM)] * len(found),
        scratch_shapes=[pltpu.SemaphoreType.DMA((len(found), PUT))],
        compiler_params=pltpu.CompilerParams(vmem_limit_bytes=2**20),
    )(*found)


def solution(mesh):
    side = math.isqrt(mesh.shape["tp"] // 2)

    def step(x, dy, gate, up, w_gate, w_up, w_down):
        tokens, width = x.shape
        hidden = gate.shape[1]
        units = tokens // ROWS * SPLIT
        cu = width // 2 // SPLIT
        cw = cu // side
        sub = ROWS // side
        out = [pltpu.VMEM(a.shape, a.dtype) for a in (x, w_gate, w_up, w_down)]
        dma = pltpu.SemaphoreType.DMA
        found = pl.pallas_call(
            functools.partial(kernel, side),
            out_shape=out,
            in_specs=[pl.BlockSpec(memory_space=pl.ANY)] * 7,
            out_specs=[pl.BlockSpec(memory_space=pltpu.VMEM)] * 4,
            scratch_shapes=[
                pltpu.VMEM((2, ROWS, width), BF16),
                pltpu.VMEM((2, ROWS, hidden), BF16),
                pltpu.VMEM((2, ROWS, hidden), BF16),
                pltpu.VMEM((tokens, 2 * hidden), BF16),
                pltpu.VMEM((hidden, tokens), BF16),
                pltpu.VMEM((2, tokens, TILE), BF16),
                pltpu.VMEM((2, tokens, TILE), BF16),
                pltpu.VMEM((SLOTS, ROWS, cu), F32),
                pltpu.VMEM((SLOTS2, ROWS, cw), F32),
                pltpu.VMEM((units, 2, ROWS // 2, cw), BF16),
                pltpu.VMEM((units, 4, ROWS // 2, cw), BF16),
                pltpu.VMEM((units, 2, sub // 2, cw), BF16),
                pltpu.VMEM((units, 4, sub // 2, cw), BF16),
                pltpu.VMEM((units, 2, sub // 2, cw), BF16),
                dma((1 + 4 * SPLIT,)),
                dma((2, 3)),
                dma((2, 2)),
                dma((10, FLIGHT)),
                dma((10, units)),
            ],
            compiler_params=pltpu.CompilerParams(
                collective_id=0, has_side_effects=True, vmem_limit_bytes=VMEM * 2**20,
            ),
        )(x, dy, gate, up, w_gate, w_up, w_down)
        return tuple(put(found))

    tokens, columns, rows = P("dp", None), P(None, "tp"), P("tp", None)
    return jax.shard_map(
        step,
        mesh=mesh,
        in_specs=(tokens, tokens, P("dp", "tp"), P("dp", "tp"), columns, columns, rows),
        out_specs=(tokens, P("dp", "tp"), P("dp", "tp"), P(("dp", "tp"), None)),
        check_vma=False,
    )
```
